32 devices in a mesh: section: 2 (over y), dp: 16 (over z, x, core).
Axes of the slice: x: 2, y: 2, z: 4, core: 2. Of those that a mesh axis runs over, the one named last changes fastest.
Arguments:
- layer_inputs: bfloat16 [2, 4096, 4096], P('section', 'dp'), may hold values from -20 to 20
- norm_gain: float32 [2, 4096], P('section'), may hold values from 0.5 to 1.5
- queries: bfloat16 [2, 4096, 2048], P('section', 'dp'), may hold values from -100 to 100
- output_gradient: bfloat16 [2, 4096, 2048], P('section', 'dp'), may hold values from -6 to 6
- w_key: bfloat16 [2, 4096, 512], P('section'), may hold values from -0.09375 to 0.09375
- value_matrix: bfloat16 [2, 4096, 512], P('section'), may hold values from -0.09375 to 0.09375
- top_grad: bfloat16 [4096, 4096], P('dp'), may hold values from -6 to 6
Outputs:
- key_grad: bfloat16 [2, 4096, 512], P('section')
- value_grad: bfloat16 [2, 4096, 512], P('section')
- input_grad: bfloat16 [2, 4096, 4096], P('section', 'dp')
The draws below stay inside these ranges and needn't reach their ends.
All inputs are finite; a program needn't handle non-finite values.
Results may differ from the reference program's by a relative error of at most 0.0082.
Values may be sent and summed in bfloat16 or wider, within the bound.
A program may use at most 128 MiB of HBM per device.

```python
import jax
import jax.numpy as jnp
from jax import lax

MODEL_WIDTH = 4096
HEAD_SIZE = 128
QUERY_HEADS = 16
KEY_VALUE_HEADS = 4
QUERY_PER_KEY = 4
SEQUENCE_TOKENS = 128
LAYERS_SECTION = 1
LAYER_TOTAL = 2
TOKEN_TOTAL = 4096
N_SECTION = 2
N_DP = 16


def draw_pair(key):
    key_inputs = jax.random.fold_in(key, 101)
    key_matrix = jax.random.fold_in(key, 102)
    inputs = jnp.clip(jax.random.normal(key_inputs, (LAYER_TOTAL, TOKEN_TOTAL, MODEL_WIDTH), jnp.float32), -6.0, 6.0)
    weight_arrays = jnp.clip(jax.random.normal(key_matrix, (LAYER_TOTAL, MODEL_WIDTH, KEY_VALUE_HEADS * HEAD_SIZE), jnp.float32), -6.0, 6.0) * MODEL_WIDTH ** (-0.5)
    return (inputs, weight_arrays)


def draw_layer_inputs(key, part):
    return draw_pair(key)[0].astype(jnp.bfloat16)


def draw_w_key(key, part):
    return draw_pair(key)[1].astype(jnp.bfloat16)


def draw_queries(key, part):
    base_draw = jnp.clip(jax.random.normal(jax.random.fold_in(key, 103), (LAYER_TOTAL, TOKEN_TOTAL, QUERY_HEADS * HEAD_SIZE), jnp.float32), -6.0, 6.0)
    return base_draw.astype(jnp.bfloat16)


def steps_of(own_key, dims, shards, smallest, largest):
    def one(dim, shards_of):
        draws = jax.random.uniform(jax.random.fold_in(jax.random.fold_in(own_key, 6), dim), (shards_of,), jnp.float32, smallest / len(shards), largest / len(shards))
        return jnp.repeat(jnp.exp(draws), dims[dim] // shards_of).reshape((-1,) + (1,) * (len(dims) - dim - 1))

    factor_of = one(*shards[0])
    for cut in shards[1:]:
        factor_of = factor_of * one(*cut)
    return factor_of


def scatter_about(rng, shape, spread, most, split=(), kind=jnp.bfloat16):
    entries = spread * jax.random.normal(rng, shape, jnp.float32)
    if split:
        entries = entries * steps_of(rng, shape, split, -0.22, 0.18)
    return jnp.clip(entries, -most, most).astype(kind)


def setup_inputs(seed: int = 0) -> dict:
    keys = jax.random.split(jax.random.key(seed), 8)
    layer_inputs = draw_layer_inputs(jax.random.fold_in(keys[7], 71), 0)
    norm_gain = jnp.clip(1.0 + 0.1 * jax.random.normal(keys[1], (LAYER_TOTAL, MODEL_WIDTH), jnp.float32), 0.5, 1.5)
    queries = draw_queries(jax.random.fold_in(keys[7], 71), 0)
    output_gradient = scatter_about(keys[3], (LAYER_TOTAL, TOKEN_TOTAL, QUERY_HEADS * HEAD_SIZE), 1.0, 6.0, ((0, 2), (1, 16)))
    w_key = draw_w_key(jax.random.fold_in(keys[7], 71), 0)
    value_matrix = scatter_about(keys[5], (LAYER_TOTAL, MODEL_WIDTH, KEY_VALUE_HEADS * HEAD_SIZE), MODEL_WIDTH ** -0.5, 0.09375, ((0, 2),))
    top_grad = scatter_about(keys[6], (TOKEN_TOTAL, MODEL_WIDTH), 1.0, 6.0, ((0, 16),))
    return {"layer_inputs": layer_inputs, "norm_gain": norm_gain, "queries": queries, "output_gradient": output_gradient, "w_key": w_key, "value_matrix": value_matrix, "top_grad": top_grad}


epsilon = 1e-05

def single_sequence(operands):
    query_sequence, key_sequence, value_sequence, sequence_output_gradient = operands
    scale = HEAD_SIZE ** (-0.5)
    heads_of_query = query_sequence.astype(jnp.float32).reshape(SEQUENCE_TOKENS, KEY_VALUE_HEADS, QUERY_PER_KEY, HEAD_SIZE)
    heads_of_key = key_sequence.astype(jnp.float32).reshape(SEQUENCE_TOKENS, KEY_VALUE_HEADS, HEAD_SIZE)
    heads_of_value = value_sequence.astype(jnp.float32).reshape(SEQUENCE_TOKENS, KEY_VALUE_HEADS, HEAD_SIZE)
    head_gradients = sequence_output_gradient.astype(jnp.float32).reshape(SEQUENCE_TOKENS, KEY_VALUE_HEADS, QUERY_PER_KEY, HEAD_SIZE)
    scores = jnp.einsum('tjgd,sjd->jgts', heads_of_query, heads_of_key) * scale
    causal = jnp.arange(SEQUENCE_TOKENS)[:, None] >= jnp.arange(SEQUENCE_TOKENS)[None, :]
    scores = jnp.where(causal, scores, -1e+30)
    row_max = lax.optimization_barrier(jnp.max(scores, axis=-1, keepdims=True))
    weight = jnp.exp(scores - row_max)
    probability = weight / lax.optimization_barrier(jnp.sum(weight, axis=-1, keepdims=True))
    prob_low = lax.optimization_barrier(probability.astype(jnp.bfloat16)).astype(jnp.float32)
    value_gradient = jnp.einsum('jgts,tjgd->sjd', prob_low, head_gradients).astype(jnp.bfloat16)
    grad_prob = jnp.einsum('tjgd,sjd->jgts', head_gradients, heads_of_value)
    row_delta = lax.optimization_barrier(jnp.sum(probability * grad_prob, axis=-1, keepdims=True))
    dscore = (probability * (grad_prob - row_delta) * scale).astype(jnp.bfloat16)
    dscore_wide = lax.optimization_barrier(dscore).astype(jnp.float32)
    key_gradient = jnp.einsum('jgts,tjgd->sjd', dscore_wide, heads_of_query).astype(jnp.bfloat16)
    return (key_gradient.reshape(SEQUENCE_TOKENS, KEY_VALUE_HEADS * HEAD_SIZE), value_gradient.reshape(SEQUENCE_TOKENS, KEY_VALUE_HEADS * HEAD_SIZE))

def reference(layer_inputs, norm_gain, queries, output_gradient, w_key, value_matrix, top_grad):
    sequence_count = TOKEN_TOTAL // SEQUENCE_TOKENS
    key_list = []
    value_list = []
    dx_list = []
    for layer_index in range(LAYER_TOTAL):
        wide_inputs = layer_inputs[layer_index].astype(jnp.float32)
        inv_rms = lax.rsqrt(lax.optimization_barrier(jnp.mean(wide_inputs * wide_inputs, axis=-1, keepdims=True)) + epsilon)
        gain_row = norm_gain[layer_index].astype(jnp.float32)
        normed = (wide_inputs * inv_rms * gain_row).astype(jnp.bfloat16)
        key_projected = jnp.dot(normed, w_key[layer_index], preferred_element_type=jnp.float32).astype(jnp.bfloat16)
        value_projected = jnp.dot(normed, value_matrix[layer_index], preferred_element_type=jnp.float32).astype(jnp.bfloat16)
        key_gradient, value_gradient = lax.map(single_sequence, (queries[layer_index].reshape(sequence_count, SEQUENCE_TOKENS, QUERY_HEADS * HEAD_SIZE), key_projected.reshape(sequence_count, SEQUENCE_TOKENS, KEY_VALUE_HEADS * HEAD_SIZE), value_projected.reshape(sequence_count, SEQUENCE_TOKENS, KEY_VALUE_HEADS * HEAD_SIZE), output_gradient[layer_index].reshape(sequence_count, SEQUENCE_TOKENS, QUERY_HEADS * HEAD_SIZE)))
        key_gradient = key_gradient.reshape(TOKEN_TOTAL, KEY_VALUE_HEADS * HEAD_SIZE)
        value_gradient = value_gradient.reshape(TOKEN_TOTAL, KEY_VALUE_HEADS * HEAD_SIZE)
        key_list.append((jnp.dot(normed.T, key_gradient, preferred_element_type=jnp.float32) / N_DP).astype(jnp.bfloat16))
        value_list.append((jnp.dot(normed.T, value_gradient, preferred_element_type=jnp.float32) / N_DP).astype(jnp.bfloat16))
        grad_norm = jnp.dot(key_gradient, w_key[layer_index].T, preferred_element_type=jnp.float32)
        grad_norm = grad_norm + jnp.dot(value_gradient, value_matrix[layer_index].T, preferred_element_type=jnp.float32)
        scaled = gain_row * grad_norm
        layer_dx = inv_rms * scaled - wide_inputs * inv_rms ** 3 * lax.optimization_barrier(jnp.mean(wide_inputs * scaled, axis=-1, keepdims=True))
        dx_list.append(layer_dx)
    carried = top_grad.astype(jnp.float32)
    section_grads = []
    for section_idx in reversed(range(N_SECTION)):
        section_total = carried
        for layer_index in range(section_idx * LAYERS_SECTION, (section_idx + 1) * LAYERS_SECTION):
            section_total = section_total + dx_list[layer_index]
        rounded = section_total.astype(jnp.bfloat16)
        section_grads.insert(0, rounded)
        carried = rounded.astype(jnp.float32)
    return (jnp.stack(key_list), jnp.stack(value_list), jnp.stack(section_grads))
```

```python
import jax
import jax.numpy as jnp
from jax import lax
from jax.experimental import pallas as pl
from jax.experimental.pallas import tpu as pltpu
from jax.sharding import PartitionSpec as P

HEAD_SIZE = 128
KEY_VALUE_HEADS = 4
SEQUENCE_TOKENS = 128


epsilon = 1e-05


def shifted(value, axis, steps):
    count = lax.axis_size(axis)
    initial, last = (max(0, -steps), min(count, count - steps))
    return lax.ppermute(value, axis, [(source, source + steps) for source in range(initial, last)])


def normalize(block_inputs, gain_row):
    wide_inputs = block_inputs.astype(jnp.float32)
    inv_rms = lax.rsqrt(jnp.mean(wide_inputs * wide_inputs, axis=-1, keepdims=True) + epsilon)
    return (wide_inputs, inv_rms, (wide_inputs * inv_rms * gain_row).astype(jnp.bfloat16))


def value_pass(heads_of_query, heads_of_key, head_gradients):
    scale = HEAD_SIZE ** (-0.5)
    scores = (
        jnp.einsum(
            "btjgd,bsjd->bjgts", heads_of_query, heads_of_key, preferred_element_type=jnp.float32
        )
        * scale
    )
    causal = lax.broadcasted_iota(
        jnp.int32, (SEQUENCE_TOKENS, SEQUENCE_TOKENS), 0
    ) >= lax.broadcasted_iota(jnp.int32, (SEQUENCE_TOKENS, SEQUENCE_TOKENS), 1)
    scores = jnp.where(causal, scores, -1e30)
    row_max = jnp.max(scores, axis=-1, keepdims=True)
    weight = jnp.exp(scores - row_max)
    probability = weight / jnp.sum(weight, axis=-1, keepdims=True)
    value_gradient = jnp.einsum(
        "bjgts,btjgd->bsjd",
        probability.astype(jnp.bfloat16),
        head_gradients,
        preferred_element_type=jnp.float32,
    )
    return (probability, value_gradient.astype(jnp.bfloat16))


def key_pass(probability, heads_of_query, heads_of_value, head_gradients):
    scale = HEAD_SIZE ** (-0.5)
    grad_prob = jnp.einsum(
        "btjgd,bsjd->bjgts", head_gradients, heads_of_value, preferred_element_type=jnp.float32
    )
    row_delta = jnp.sum(probability * grad_prob, axis=-1, keepdims=True)
    dscore = (probability * (grad_prob - row_delta) * scale).astype(jnp.bfloat16)
    key_gradient = jnp.einsum(
        "bjgts,btjgd->bsjd", dscore, heads_of_query, preferred_element_type=jnp.float32
    )
    return key_gradient.astype(jnp.bfloat16)


def weight_term(normed, grad_proj):
    return jnp.einsum("td,tk->dk", normed, grad_proj, preferred_element_type=jnp.float32)


def input_term(
    wide_inputs, inv_rms, gain_row, key_gradient, value_gradient, key_weight, value_weight
):
    grad_norm = jnp.einsum(
        "tk,dk->td", key_gradient, key_weight, preferred_element_type=jnp.float32
    )
    grad_norm = grad_norm + jnp.einsum(
        "tk,dk->td", value_gradient, value_weight, preferred_element_type=jnp.float32
    )
    scaled = gain_row * grad_norm
    return inv_rms * scaled - wide_inputs * inv_rms**3 * jnp.mean(
        wide_inputs * scaled, axis=-1, keepdims=True
    )


def layer_grads(
    block_inputs,
    gain_row,
    block_query_rows,
    block_output_gradient,
    key_weight,
    value_weight,
):
    wide_inputs, inv_rms, normed = normalize(block_inputs, gain_row)
    key_projected = jnp.dot(normed, key_weight, preferred_element_type=jnp.float32).astype(
        jnp.bfloat16
    )
    value_projected = jnp.dot(normed, value_weight, preferred_element_type=jnp.float32).astype(
        jnp.bfloat16
    )
    count_of_rows = block_inputs.shape[0]
    sequence_count = count_of_rows // SEQUENCE_TOKENS
    heads_of_query = block_query_rows.reshape(
        sequence_count, SEQUENCE_TOKENS, KEY_VALUE_HEADS, -1, HEAD_SIZE
    )
    head_gradients = block_output_gradient.reshape(
        sequence_count, SEQUENCE_TOKENS, KEY_VALUE_HEADS, -1, HEAD_SIZE
    )
    heads_of_key = key_projected.reshape(
        sequence_count, SEQUENCE_TOKENS, KEY_VALUE_HEADS, HEAD_SIZE
    )
    heads_of_value = value_projected.reshape(
        sequence_count, SEQUENCE_TOKENS, KEY_VALUE_HEADS, HEAD_SIZE
    )
    probability, value_gradient = value_pass(heads_of_query, heads_of_key, head_gradients)
    value_gradient = value_gradient.reshape(count_of_rows, KEY_VALUE_HEADS * HEAD_SIZE)
    value_partial = weight_term(normed, value_gradient)
    key_gradient = key_pass(probability, heads_of_query, heads_of_value, head_gradients).reshape(
        count_of_rows, KEY_VALUE_HEADS * HEAD_SIZE
    )
    key_partial = weight_term(normed, key_gradient)
    layer_dx = input_term(
        wide_inputs, inv_rms, gain_row, key_gradient, value_gradient, key_weight, value_weight
    )
    return (key_partial, value_partial, layer_dx)


CHUNKS_PER_ARRAY = 4


def bit_orders(bit_count, chunk_count):
    plain = list(range(bit_count))
    swapped = list(plain)
    if bit_count >= 3:
        swapped[1], swapped[2] = swapped[2], swapped[1]
    return [swapped if chunk % 4 == 3 else plain for chunk in range(chunk_count)]


def exchange_kernel(
    replicas,
    sections,
    key_in,
    value_in,
    cotangent_in,
    key_out,
    value_out,
    cotangent_out,
    held,
    gathered,
    *rest,
):
    bit_count = replicas.bit_length() - 1
    landing = rest[:bit_count]
    send_sem, recv_sem, load_sem, store_sem, cot_sem = rest[bit_count:]
    rows = key_in.shape[0]
    chunk_rows = rows // CHUNKS_PER_ARRAY
    chunk_count = 2 * CHUNKS_PER_ARRAY
    stage_count = 2 * bit_count
    orders = bit_orders(bit_count, chunk_count)
    section = lax.axis_index("section")
    me = lax.axis_index("dp")
    below = lax.rem(section + sections - 1, sections)
    above = lax.rem(section + 1, sections)
    partners = []
    bits = []
    for bit in range(bit_count):
        value = lax.rem(me // (1 << bit), 2)
        bits.append(value)
        partners.append(me + (1 - 2 * value) * (1 << bit))

    barrier = pltpu.get_barrier_semaphore()
    for partner in partners:
        pl.semaphore_signal(
            barrier, inc=1, device_id=(section, partner), device_id_type=pl.DeviceIdType.MESH
        )
    for neighbour in (below, above):
        pl.semaphore_signal(
            barrier, inc=1, device_id=(neighbour, me), device_id_type=pl.DeviceIdType.MESH
        )
    pl.semaphore_wait(barrier, bit_count + 2)

    cot_copy = pltpu.make_async_remote_copy(
        src_ref=cotangent_in,
        dst_ref=cotangent_out,
        send_sem=cot_sem.at[0],
        recv_sem=cot_sem.at[1],
        device_id=(below, me),
        device_id_type=pl.DeviceIdType.MESH,
    )

    def source(chunk):
        return (value_in, key_in)[chunk // CHUNKS_PER_ARRAY]

    def target(chunk):
        return (value_out, key_out)[chunk // CHUNKS_PER_ARRAY]

    def base(chunk):
        return (chunk % CHUNKS_PER_ARRAY) * chunk_rows

    offsets = []
    for chunk in range(chunk_count):
        offset = base(chunk)
        kept = [offset]
        for stage, bit in enumerate(orders[chunk]):
            offset = offset + bits[bit] * (chunk_rows >> (stage + 1))
            kept.append(offset)
        offsets.append(kept)

    def area(chunk, offset, size, buffer=held):
        return buffer.at[chunk // CHUNKS_PER_ARRAY, pl.ds(pl.multiple_of(offset, 16), size)]

    def load_copy(chunk):
        half = chunk_rows // 2
        start = pl.multiple_of(offsets[chunk][1], 16)
        return pltpu.make_async_copy(
            source(chunk).at[pl.ds(start, half)],
            area(chunk, offsets[chunk][1], half),
            load_sem.at[chunk],
        )

    def stage_copy(chunk, stage):
        if stage < bit_count:
            bit = orders[chunk][stage]
            size = chunk_rows >> (stage + 1)
            other = offsets[chunk][stage] + (1 - bits[bit]) * size
            if stage == 0:
                src = source(chunk).at[pl.ds(pl.multiple_of(other, 16), size)]
            else:
                src = area(chunk, other, size)
            dst = landing[stage].at[pl.ds(chunk * size, size)]
        else:
            level = stage_count - 1 - stage
            bit = orders[chunk][level]
            size = chunk_rows >> (level + 1)
            src = area(chunk, offsets[chunk][level + 1], size, gathered)
            dst = area(chunk, offsets[chunk][level + 1], size, gathered)
        return pltpu.make_async_remote_copy(
            src_ref=src,
            dst_ref=dst,
            send_sem=send_sem.at[chunk, stage],
            recv_sem=recv_sem.at[chunk, stage],
            device_id=(section, partners[bit]),
            device_id_type=pl.DeviceIdType.MESH,
        )

    def store_copy(chunk):
        return pltpu.make_async_copy(
            area(chunk, base(chunk), chunk_rows, gathered),
            target(chunk).at[pl.ds(base(chunk), chunk_rows)],
            store_sem.at[chunk],
        )

    def add(chunk, stage):
        size = chunk_rows >> (stage + 1)
        tile = min(size, 32)
        index = chunk // CHUNKS_PER_ARRAY
        start = offsets[chunk][stage + 1]
        is_final = stage == bit_count - 1
        result = gathered if is_final else held

        @pl.loop(0, size // tile)
        def _(step):
            here = pl.ds(pl.multiple_of(start + step * tile, 16), tile)
            there = pl.ds(pl.multiple_of(chunk * size + step * tile, 16), tile)
            total = held[index, here].astype(jnp.float32) + landing[stage][there].astype(
                jnp.float32
            )
            if is_final:
                total = total * (1.0 / replicas)
            result[index, here] = total.astype(jnp.bfloat16)

    def finish(chunk, stage):
        if stage == 0:
            load_copy(chunk).wait()
        stage_copy(chunk, stage).wait()
        if stage < bit_count:
            add(chunk, stage)
        if stage + 1 < stage_count:
            stage_copy(chunk, stage + 1).start()
        else:
            store_copy(chunk).start()

    for chunk in range(chunk_count):
        stage_copy(chunk, 0).start()
        load_copy(chunk).start()
    cot_copy.start()
    lags = [stage + (2 if stage else 0) for stage in range(stage_count)]
    for step in range(chunk_count + lags[-1]):
        for stage in reversed(range(stage_count)):
            chunk = step - lags[stage]
            if 0 <= chunk < chunk_count:
                finish(chunk, stage)
    cot_copy.wait()
    for chunk in range(chunk_count):
        store_copy(chunk).wait()


def exchange(key_partial, value_partial, cotangent):
    replicas = lax.axis_size("dp")
    sections = lax.axis_size("section")
    rows, columns = key_partial.shape
    bit_count = replicas.bit_length() - 1
    chunk_count = 2 * CHUNKS_PER_ARRAY
    kind = key_partial.dtype
    anywhere = pl.BlockSpec(memory_space=pl.ANY)
    return pl.pallas_call(
        lambda *refs: exchange_kernel(replicas, sections, *refs),
        out_shape=(
            jax.ShapeDtypeStruct(key_partial.shape, kind),
            jax.ShapeDtypeStruct(value_partial.shape, kind),
            jax.ShapeDtypeStruct(cotangent.shape, cotangent.dtype),
        ),
        in_specs=[anywhere] * 3,
        out_specs=(anywhere,) * 3,
        scratch_shapes=[pltpu.VMEM((2, rows, columns), kind)] * 2
        + [
            pltpu.VMEM((2 * rows >> (stage + 1), columns), kind) for stage in range(bit_count)
        ]
        + [
            pltpu.SemaphoreType.DMA((chunk_count, 2 * bit_count)),
            pltpu.SemaphoreType.DMA((chunk_count, 2 * bit_count)),
            pltpu.SemaphoreType.DMA((chunk_count,)),
            pltpu.SemaphoreType.DMA((chunk_count,)),
            pltpu.SemaphoreType.DMA((2,)),
        ],
        compiler_params=pltpu.CompilerParams(
            collective_id=0, has_side_effects=True, vmem_limit_bytes=32 * 1024 * 1024
        ),
    )(key_partial, value_partial, cotangent)


def per_device(layer_inputs, norm_gain, queries, output_gradient, w_key, value_matrix, top_grad):
    is_last = lax.axis_index("section") == lax.axis_size("section") - 1
    key_partial, value_partial, layer_dx = layer_grads(
        layer_inputs[0],
        norm_gain[0],
        queries[0],
        output_gradient[0],
        w_key[0],
        value_matrix[0],
    )
    own_total = layer_dx + jnp.where(is_last, top_grad.astype(jnp.float32), 0.0)
    key_grad, value_grad, received = exchange(
        key_partial.astype(jnp.bfloat16),
        value_partial.astype(jnp.bfloat16),
        own_total.astype(jnp.bfloat16),
    )
    received = jnp.where(is_last, 0.0, received.astype(jnp.float32))
    input_grad = (received + own_total).astype(jnp.bfloat16)
    return (key_grad[None], value_grad[None], input_grad[None])


def solution(mesh):
    in_specs = (
        P("section", "dp", None),
        P("section", None),
        P("section", "dp", None),
        P("section", "dp", None),
        P("section", None, None),
        P("section", None, None),
        P("dp", None),
    )
    out_specs = (P("section", None, None), P("section", None, None), P("section", "dp", None))
    return jax.shard_map(
        per_device, mesh=mesh, in_specs=in_specs, out_specs=out_specs, check_vma=False
    )
```

```python
import jax
import jax.numpy as jnp
from jax import lax
from jax.experimental import pallas as pl
from jax.experimental.pallas import tpu as pltpu
from jax.sharding import PartitionSpec as P

HEAD_SIZE = 128
KEY_VALUE_HEADS = 4
SEQUENCE_TOKENS = 128


epsilon = 1e-05


CHUNKS_PER_ARRAY = 4


def bit_orders(bit_count, chunk_count):
    plain = list(range(bit_count))
    swapped = list(plain)
    if bit_count >= 3:
        swapped[1], swapped[2] = swapped[2], swapped[1]
    return [swapped if chunk % 4 == 3 else plain for chunk in range(chunk_count)]


MESH = pl.DeviceIdType.MESH
FEATURE_BLOCK = 512
TERM_BLOCK = 256
ROW_TILE = 16
LOAD_PIECES = 4
INPUT_TERM_STEP = 3
FINAL_SUM_STEP = 10


def contract(left, right, left_axis, right_axis):
    return lax.dot_general(
        left, right, (((left_axis,), (right_axis,)), ((), ())), preferred_element_type=jnp.float32
    )


def whole_kernel(
    replicas,
    sections,
    x_in,
    gain,
    query_in,
    gradient_in,
    key_weight_in,
    value_weight_in,
    top_in,
    key_out,
    value_out,
    input_out,
    x_held,
    normed,
    inv_rms,
    query,
    gradient,
    weights,
    top,
    projected_wide,
    projected,
    grads,
    scaled,
    row_dot,
    outgoing,
    received,
    final,
    held,
    gathered,
    *rest,
):
    bit_count = replicas.bit_length() - 1
    landing = rest[:bit_count]
    send_sem, recv_sem, store_sem, cot_sem, x_sem, weight_sem, load_sem = rest[bit_count:]
    rows = key_out.shape[1]
    tokens = x_held.shape[0]
    width = x_held.shape[1]
    group = query.shape[1] // KEY_VALUE_HEADS
    scale = HEAD_SIZE ** (-0.5)
    chunk_rows = rows // CHUNKS_PER_ARRAY
    chunk_count = 2 * CHUNKS_PER_ARRAY
    stage_count = 2 * bit_count
    orders = bit_orders(bit_count, chunk_count)
    section = lax.axis_index("section")
    me = lax.axis_index("dp")
    below = lax.rem(section + sections - 1, sections)
    above = lax.rem(section + 1, sections)
    partners = []
    bits = []
    for bit in range(bit_count):
        value = lax.rem(me // (1 << bit), 2)
        bits.append(value)
        partners.append(me + (1 - 2 * value) * (1 << bit))

    piece = tokens // LOAD_PIECES

    def x_copy(index):
        here = pl.ds(index * piece, piece)
        return pltpu.make_async_copy(x_in.at[0, here], x_held.at[here], x_sem.at[index])

    def weight_copy(which, block):
        here = pl.ds(pl.multiple_of(block * FEATURE_BLOCK, FEATURE_BLOCK), FEATURE_BLOCK)
        return pltpu.make_async_copy(
            (key_weight_in, value_weight_in)[which].at[0, here],
            weights.at[which, here],
            weight_sem.at[which, block],
        )

    query_copy = pltpu.make_async_copy(query_in.at[0], query, load_sem.at[0])
    gradient_copy = pltpu.make_async_copy(gradient_in.at[0], gradient, load_sem.at[1])
    top_copy = pltpu.make_async_copy(top_in, top, load_sem.at[2])
    feature_blocks = width // FEATURE_BLOCK
    for index in range(LOAD_PIECES):
        x_copy(index).start()
    for block in range(feature_blocks):
        for which in range(2):
            weight_copy(which, block).start()
    query_copy.start()
    gradient_copy.start()

    barrier = pltpu.get_barrier_semaphore()
    for partner in partners:
        pl.semaphore_signal(
            barrier, inc=1, device_id=(section, partner), device_id_type=MESH
        )
    for neighbour in (below, above):
        pl.semaphore_signal(
            barrier, inc=1, device_id=(neighbour, me), device_id_type=MESH
        )

    for index in range(LOAD_PIECES):
        x_copy(index).wait()

        @pl.loop(0, piece // ROW_TILE)
        def _(step):
            here = pl.ds(pl.multiple_of(index * piece + step * ROW_TILE, ROW_TILE), ROW_TILE)
            wide = x_held[here].astype(jnp.float32)
            inverse = lax.rsqrt(jnp.mean(wide * wide, axis=-1, keepdims=True) + epsilon)
            inv_rms[here] = inverse
            normed[here] = (wide * inverse * gain[...]).astype(jnp.bfloat16)

    projected_wide[...] = jnp.zeros_like(projected_wide)

    @pl.loop(0, feature_blocks)
    def _(block):
        here = pl.ds(pl.multiple_of(block * FEATURE_BLOCK, FEATURE_BLOCK), FEATURE_BLOCK)
        for which in range(2):
            weight_copy(which, block).wait()
            projected_wide[which] += contract(normed[:, here], weights[which, here], 1, 0)

    projected[...] = projected_wide[...].astype(jnp.bfloat16)
    query_copy.wait()
    gradient_copy.wait()
    top_copy.start()

    @pl.loop(0, tokens // SEQUENCE_TOKENS * KEY_VALUE_HEADS)
    def _(index):
        sequence = index // KEY_VALUE_HEADS
        head = lax.rem(index, KEY_VALUE_HEADS)
        here = pl.ds(pl.multiple_of(sequence * SEQUENCE_TOKENS, SEQUENCE_TOKENS), SEQUENCE_TOKENS)
        column = pl.ds(pl.multiple_of(head * HEAD_SIZE, HEAD_SIZE), HEAD_SIZE)

        def stacked(ref):
            return jnp.concatenate(
                [
                    ref[here, pl.ds(pl.multiple_of(head * group + part, HEAD_SIZE), HEAD_SIZE)]
                    for part in range(0, group, HEAD_SIZE)
                ],
                axis=0,
            )

        head_queries = stacked(query)
        head_gradients = stacked(gradient)
        scores = contract(head_queries, projected[0, here, column], 1, 1) * scale
        query_row = lax.rem(lax.broadcasted_iota(jnp.int32, scores.shape, 0), SEQUENCE_TOKENS)
        key_row = lax.broadcasted_iota(jnp.int32, scores.shape, 1)
        scores = jnp.where(query_row >= key_row, scores, -1e30)
        weight = jnp.exp(scores - jnp.max(scores, axis=-1, keepdims=True))
        probability = weight * (1.0 / jnp.sum(weight, axis=-1, keepdims=True))
        grads[1, here, column] = contract(
            probability.astype(jnp.bfloat16), head_gradients, 0, 0
        ).astype(jnp.bfloat16)
        grad_prob = contract(head_gradients, projected[1, here, column], 1, 1)
        row_delta = jnp.sum(probability * grad_prob, axis=-1, keepdims=True)
        dscore = (probability * (grad_prob - row_delta) * scale).astype(jnp.bfloat16)
        grads[0, here, column] = contract(dscore, head_queries, 0, 0).astype(jnp.bfloat16)

    pl.semaphore_wait(barrier, bit_count + 2)

    cot_copy = pltpu.make_async_remote_copy(
        src_ref=outgoing,
        dst_ref=received,
        send_sem=cot_sem.at[0],
        recv_sem=cot_sem.at[1],
        device_id=(below, me),
        device_id_type=MESH,
    )

    def target(chunk):
        return (value_out, key_out)[chunk // CHUNKS_PER_ARRAY]

    def base(chunk):
        return (chunk % CHUNKS_PER_ARRAY) * chunk_rows

    offsets = []
    for chunk in range(chunk_count):
        offset = base(chunk)
        kept = [offset]
        for stage, bit in enumerate(orders[chunk]):
            offset = offset + bits[bit] * (chunk_rows >> (stage + 1))
            kept.append(offset)
        offsets.append(kept)

    def area(chunk, offset, size, buffer=held):
        return buffer.at[chunk // CHUNKS_PER_ARRAY, pl.ds(pl.multiple_of(offset, 16), size)]

    def stage_copy(chunk, stage):
        if stage < bit_count:
            bit = orders[chunk][stage]
            size = chunk_rows >> (stage + 1)
            other = offsets[chunk][stage] + (1 - bits[bit]) * size
            src = area(chunk, other, size)
            dst = landing[stage].at[pl.ds(chunk * size, size)]
        else:
            level = stage_count - 1 - stage
            bit = orders[chunk][level]
            size = chunk_rows >> (level + 1)
            src = area(chunk, offsets[chunk][level + 1], size, gathered)
            dst = area(chunk, offsets[chunk][level + 1], size, gathered)
        return pltpu.make_async_remote_copy(
            src_ref=src,
            dst_ref=dst,
            send_sem=send_sem.at[chunk, stage],
            recv_sem=recv_sem.at[chunk, stage],
            device_id=(section, partners[bit]),
            device_id_type=MESH,
        )

    def store_copy(chunk):
        return pltpu.make_async_copy(
            area(chunk, base(chunk), chunk_rows, gathered),
            target(chunk).at[0, pl.ds(base(chunk), chunk_rows)],
            store_sem.at[chunk],
        )

    def add(chunk, stage):
        size = chunk_rows >> (stage + 1)
        tile = min(size, 32)
        index = chunk // CHUNKS_PER_ARRAY
        start = offsets[chunk][stage + 1]
        is_final = stage == bit_count - 1
        result = gathered if is_final else held

        @pl.loop(0, size // tile)
        def _(step):
            here = pl.ds(pl.multiple_of(start + step * tile, 16), tile)
            there = pl.ds(pl.multiple_of(chunk * size + step * tile, 16), tile)
            total = held[index, here].astype(jnp.float32) + landing[stage][there].astype(
                jnp.float32
            )
            if is_final:
                total = total * (1.0 / replicas)
            result[index, here] = total.astype(jnp.bfloat16)

    def finish(chunk, stage):
        stage_copy(chunk, stage).wait()
        if stage < bit_count:
            add(chunk, stage)
        if stage + 1 < stage_count:
            stage_copy(chunk, stage + 1).start()
        else:
            store_copy(chunk).start()

    def weight_term(chunk):
        which = 1 - chunk // CHUNKS_PER_ARRAY
        index = chunk // CHUNKS_PER_ARRAY

        @pl.loop(0, chunk_rows // TERM_BLOCK)
        def _(step):
            here = pl.ds(
                pl.multiple_of(base(chunk) + step * TERM_BLOCK, TERM_BLOCK), TERM_BLOCK
            )
            term = contract(normed[:, here], grads[which], 0, 0)
            held[index, here] = term.astype(jnp.bfloat16)

    is_last = jnp.where(section == sections - 1, 1.0, 0.0)

    def input_term():
        row_dot[...] = jnp.zeros_like(row_dot)

        @pl.loop(0, feature_blocks)
        def _(block):
            here = pl.ds(pl.multiple_of(block * FEATURE_BLOCK, FEATURE_BLOCK), FEATURE_BLOCK)
            grad_norm = contract(grads[0], weights[0, here], 1, 1)
            grad_norm = grad_norm + contract(grads[1], weights[1, here], 1, 1)
            part = gain[:, here] * grad_norm
            scaled[:, here] = part
            row_dot[...] += jnp.sum(
                x_held[:, here].astype(jnp.float32) * part, axis=-1, keepdims=True
            )

        top_copy.wait()

        @pl.loop(0, tokens // ROW_TILE)
        def _(step):
            here = pl.ds(pl.multiple_of(step * ROW_TILE, ROW_TILE), ROW_TILE)
            inverse = inv_rms[here]
            pull = inverse * inverse * inverse * (row_dot[here] * (1.0 / width))
            total = inverse * scaled[here] - x_held[here].astype(jnp.float32) * pull
            total = total + top[here].astype(jnp.float32) * is_last
            scaled[here] = total
            outgoing[here] = total.astype(jnp.bfloat16)

        cot_copy.start()

    final_copy = pltpu.make_async_copy(final, input_out.at[0], load_sem.at[3])

    def final_sum():
        cot_copy.wait()

        @pl.loop(0, tokens // ROW_TILE)
        def _(step):
            here = pl.ds(pl.multiple_of(step * ROW_TILE, ROW_TILE), ROW_TILE)
            total = scaled[here] + received[here].astype(jnp.float32) * (1.0 - is_last)
            final[here] = total.astype(jnp.bfloat16)

        final_copy.start()

    lags = [stage + (2 if stage else 1) for stage in range(stage_count)]
    for step in range(chunk_count + lags[-1]):
        for stage in reversed(range(stage_count)):
            chunk = step - lags[stage]
            if 0 <= chunk < chunk_count:
                finish(chunk, stage)
        if step < chunk_count:
            weight_term(step)
            stage_copy(step, 0).start()
        if step == INPUT_TERM_STEP:
            input_term()
        if step == FINAL_SUM_STEP:
            final_sum()
    final_copy.wait()
    for chunk in range(chunk_count):
        store_copy(chunk).wait()


def per_device(layer_inputs, norm_gain, queries, output_gradient, w_key, value_matrix, top_grad):
    replicas = lax.axis_size("dp")
    sections = lax.axis_size("section")
    tokens, width = layer_inputs.shape[1:]
    rows, columns = w_key.shape[1:]
    bit_count = replicas.bit_length() - 1
    chunk_count = 2 * CHUNKS_PER_ARRAY
    low = jnp.bfloat16
    wide = jnp.float32
    anywhere = pl.BlockSpec(memory_space=pl.ANY)
    whole = pl.BlockSpec(memory_space=pltpu.VMEM)
    return pl.pallas_call(
        lambda *refs: whole_kernel(replicas, sections, *refs),
        out_shape=(
            jax.ShapeDtypeStruct(w_key.shape, low),
            jax.ShapeDtypeStruct(value_matrix.shape, low),
            jax.ShapeDtypeStruct(layer_inputs.shape, low),
        ),
        in_specs=[anywhere, whole] + [anywhere] * 5,
        out_specs=(anywhere,) * 3,
        scratch_shapes=[
            pltpu.VMEM((tokens, width), low),
            pltpu.VMEM((tokens, width), low),
            pltpu.VMEM((tokens, 1), wide),
            pltpu.VMEM(queries.shape[1:], low),
            pltpu.VMEM(queries.shape[1:], low),
            pltpu.VMEM((2, rows, columns), low),
            pltpu.VMEM((tokens, width), low),
            pltpu.VMEM((2, tokens, columns), wide),
            pltpu.VMEM((2, tokens, columns), low),
            pltpu.VMEM((2, tokens, columns), low),
            pltpu.VMEM((tokens, width), wide),
            pltpu.VMEM((tokens, 1), wide),
            pltpu.VMEM((tokens, width), low),
            pltpu.VMEM((tokens, width), low),
            pltpu.VMEM((tokens, width), low),
            pltpu.VMEM((2, rows, columns), low),
            pltpu.VMEM((2, rows, columns), low),
        ]
        + [pltpu.VMEM((2 * rows >> (stage + 1), columns), low) for stage in range(bit_count)]
        + [
            pltpu.SemaphoreType.DMA((chunk_count, 2 * bit_count)),
            pltpu.SemaphoreType.DMA((chunk_count, 2 * bit_count)),
            pltpu.SemaphoreType.DMA((chunk_count,)),
            pltpu.SemaphoreType.DMA((2,)),
            pltpu.SemaphoreType.DMA((LOAD_PIECES,)),
            pltpu.SemaphoreType.DMA((2, width // FEATURE_BLOCK)),
            pltpu.SemaphoreType.DMA((4,)),
        ],
        compiler_params=pltpu.CompilerParams(
            collective_id=0, has_side_effects=True, vmem_limit_bytes=60 * 1024 * 1024
        ),
    )(layer_inputs, norm_gain, queries, output_gradient, w_key, value_matrix, top_grad)


def solution(mesh):
    in_specs = (
        P("section", "dp", None),
        P("section", None),
        P("section", "dp", None),
        P("section", "dp", None),
        P("section", None, None),
        P("section", None, None),
        P("dp", None),
    )
    out_specs = (P("section", None, None), P("section", None, None), P("section", "dp", None))
    return jax.shard_map(
        per_device, mesh=mesh, in_specs=in_specs, out_specs=out_specs, check_vma=False
    )
```

```python
import jax
import jax.numpy as jnp
from jax import lax
from jax.experimental import pallas as pl
from jax.experimental.pallas import tpu as pltpu
from jax.sharding import PartitionSpec as P

HEAD_SIZE = 128
KEY_VALUE_HEADS = 4
SEQUENCE_TOKENS = 128


epsilon = 1e-05


MOST_CHUNKS = 8


MESH = pl.DeviceIdType.MESH
FEATURE_BLOCK = 512
TERM_BLOCK = 256
ROW_TILE = 16
LOAD_PIECES = 4
KEY_PASS_STEP = 3
INPUT_TERM_STEP = 6
FINAL_SUM_STEP = 20


def chunks_of(rows, replicas):
    return min(MOST_CHUNKS, rows // (ROW_TILE * replicas))


def contract(left, right, left_axis, right_axis):
    return lax.dot_general(
        left, right, (((left_axis,), (right_axis,)), ((), ())), preferred_element_type=jnp.float32
    )


def whole_kernel(
    replicas,
    sections,
    x_in,
    gain,
    query_in,
    gradient_in,
    key_weight_in,
    value_weight_in,
    top_in,
    key_out,
    value_out,
    input_out,
    x_held,
    normed,
    inv_rms,
    query,
    gradient,
    weights,
    top,
    projected_wide,
    projected,
    grads,
    scaled,
    row_dot,
    probabilities,
    outgoing,
    received,
    final,
    held,
    gathered,
    *rest,
):
    bit_count = replicas.bit_length() - 1
    landing = rest[:bit_count]
    send_sem, recv_sem, store_sem, cot_sem, x_sem, weight_sem, load_sem = rest[bit_count:]
    rows = key_out.shape[1]
    chunks_per_array = chunks_of(rows, replicas)
    tokens = x_held.shape[0]
    width = x_held.shape[1]
    group = query.shape[1] // KEY_VALUE_HEADS
    scale = HEAD_SIZE ** (-0.5)
    chunk_rows = rows // chunks_per_array
    chunk_count = 2 * chunks_per_array
    stage_count = 2 * bit_count
    orders = [list(range(bit_count))] * chunk_count
    section = lax.axis_index("section")
    me = lax.axis_index("dp")
    below = lax.rem(section + sections - 1, sections)
    above = lax.rem(section + 1, sections)
    partners = []
    bits = []
    for bit in range(bit_count):
        value = lax.rem(me // (1 << bit), 2)
        bits.append(value)
        partners.append(me + (1 - 2 * value) * (1 << bit))

    piece = tokens // LOAD_PIECES

    def x_copy(index):
        here = pl.ds(index * piece, piece)
        return pltpu.make_async_copy(x_in.at[0, here], x_held.at[here], x_sem.at[index])

    def weight_copy(which, block):
        here = pl.ds(pl.multiple_of(block * FEATURE_BLOCK, FEATURE_BLOCK), FEATURE_BLOCK)
        return pltpu.make_async_copy(
            (key_weight_in, value_weight_in)[which].at[0, here],
            weights.at[which, here],
            weight_sem.at[which, block],
        )

    query_copy = pltpu.make_async_copy(query_in.at[0], query, load_sem.at[0])
    gradient_copy = pltpu.make_async_copy(gradient_in.at[0], gradient, load_sem.at[1])
    top_copy = pltpu.make_async_copy(top_in, top, load_sem.at[2])
    feature_blocks = width // FEATURE_BLOCK
    for index in range(LOAD_PIECES):
        x_copy(index).start()
    for block in range(feature_blocks):
        weight_copy(0, block).start()
    query_copy.start()
    gradient_copy.start()
    for block in range(feature_blocks):
        weight_copy(1, block).start()

    barrier = pltpu.get_barrier_semaphore()
    for partner in partners:
        pl.semaphore_signal(
            barrier, inc=1, device_id=(section, partner), device_id_type=MESH
        )
    for neighbour in (below, above):
        pl.semaphore_signal(
            barrier, inc=1, device_id=(neighbour, me), device_id_type=MESH
        )

    for index in range(LOAD_PIECES):
        x_copy(index).wait()

        @pl.loop(0, piece // ROW_TILE)
        def _(step):
            here = pl.ds(pl.multiple_of(index * piece + step * ROW_TILE, ROW_TILE), ROW_TILE)
            wide = x_held[here].astype(jnp.float32)
            inverse = lax.rsqrt(jnp.mean(wide * wide, axis=-1, keepdims=True) + epsilon)
            inv_rms[here] = inverse
            normed[here] = (wide * inverse * gain[...]).astype(jnp.bfloat16)

    def project(which):
        projected_wide[...] = jnp.zeros_like(projected_wide)

        @pl.loop(0, feature_blocks)
        def _(block):
            here = pl.ds(pl.multiple_of(block * FEATURE_BLOCK, FEATURE_BLOCK), FEATURE_BLOCK)
            weight_copy(which, block).wait()
            projected_wide[...] += contract(normed[:, here], weights[which, here], 1, 0)

        projected[which] = projected_wide[...].astype(jnp.bfloat16)

    def places(index):
        sequence = index // KEY_VALUE_HEADS
        head = lax.rem(index, KEY_VALUE_HEADS)
        here = pl.ds(pl.multiple_of(sequence * SEQUENCE_TOKENS, SEQUENCE_TOKENS), SEQUENCE_TOKENS)
        column = pl.ds(pl.multiple_of(head * HEAD_SIZE, HEAD_SIZE), HEAD_SIZE)

        def stacked(ref):
            return jnp.concatenate(
                [
                    ref[here, pl.ds(pl.multiple_of(head * group + part, HEAD_SIZE), HEAD_SIZE)]
                    for part in range(0, group, HEAD_SIZE)
                ],
                axis=0,
            )

        return here, column, stacked

    head_count = tokens // SEQUENCE_TOKENS * KEY_VALUE_HEADS

    def value_pass():
        @pl.loop(0, head_count)
        def _(index):
            here, column, stacked = places(index)
            scores = contract(stacked(query), projected[0, here, column], 1, 1) * scale
            query_row = lax.rem(lax.broadcasted_iota(jnp.int32, scores.shape, 0), SEQUENCE_TOKENS)
            key_row = lax.broadcasted_iota(jnp.int32, scores.shape, 1)
            scores = jnp.where(query_row >= key_row, scores, -1e30)
            weight = jnp.exp(scores - jnp.max(scores, axis=-1, keepdims=True))
            probability = weight * (1.0 / jnp.sum(weight, axis=-1, keepdims=True))
            probabilities[index] = probability
            grads[1, here, column] = contract(
                probability.astype(jnp.bfloat16), stacked(gradient), 0, 0
            ).astype(jnp.bfloat16)

    def key_pass():
        @pl.loop(0, head_count)
        def _(index):
            here, column, stacked = places(index)
            probability = probabilities[index]
            grad_prob = contract(stacked(gradient), projected[1, here, column], 1, 1)
            row_delta = jnp.sum(probability * grad_prob, axis=-1, keepdims=True)
            dscore = (probability * (grad_prob - row_delta) * scale).astype(jnp.bfloat16)
            grads[0, here, column] = contract(dscore, stacked(query), 0, 0).astype(jnp.bfloat16)

    project(0)
    query_copy.wait()
    gradient_copy.wait()
    value_pass()
    top_copy.start()

    pl.semaphore_wait(barrier, bit_count + 2)

    cot_copy = pltpu.make_async_remote_copy(
        src_ref=outgoing,
        dst_ref=received,
        send_sem=cot_sem.at[0],
        recv_sem=cot_sem.at[1],
        device_id=(below, me),
        device_id_type=MESH,
    )

    def target(chunk):
        return (value_out, key_out)[chunk // chunks_per_array]

    def base(chunk):
        return (chunk % chunks_per_array) * chunk_rows

    offsets = []
    for chunk in range(chunk_count):
        offset = base(chunk)
        kept = [offset]
        for stage, bit in enumerate(orders[chunk]):
            offset = offset + bits[bit] * (chunk_rows >> (stage + 1))
            kept.append(offset)
        offsets.append(kept)

    def area(chunk, offset, size, buffer=held):
        return buffer.at[chunk // chunks_per_array, pl.ds(pl.multiple_of(offset, 16), size)]

    def stage_copy(chunk, stage):
        if stage < bit_count:
            bit = orders[chunk][stage]
            size = chunk_rows >> (stage + 1)
            other = offsets[chunk][stage] + (1 - bits[bit]) * size
            src = area(chunk, other, size)
            dst = landing[stage].at[pl.ds(chunk * size, size)]
        else:
            level = stage_count - 1 - stage
            bit = orders[chunk][level]
            size = chunk_rows >> (level + 1)
            src = area(chunk, offsets[chunk][level + 1], size, gathered)
            dst = area(chunk, offsets[chunk][level + 1], size, gathered)
        return pltpu.make_async_remote_copy(
            src_ref=src,
            dst_ref=dst,
            send_sem=send_sem.at[chunk, stage],
            recv_sem=recv_sem.at[chunk, stage],
            device_id=(section, partners[bit]),
            device_id_type=MESH,
        )

    def store_copy(chunk):
        return pltpu.make_async_copy(
            area(chunk, base(chunk), chunk_rows, gathered),
            target(chunk).at[0, pl.ds(base(chunk), chunk_rows)],
            store_sem.at[chunk],
        )

    def add(chunk, stage):
        size = chunk_rows >> (stage + 1)
        tile = min(size, 32)
        index = chunk // chunks_per_array
        start = offsets[chunk][stage + 1]
        is_final = stage == bit_count - 1
        result = gathered if is_final else held

        @pl.loop(0, size // tile)
        def _(step):
            here = pl.ds(pl.multiple_of(start + step * tile, 16), tile)
            there = pl.ds(pl.multiple_of(chunk * size + step * tile, 16), tile)
            total = held[index, here].astype(jnp.float32) + landing[stage][there].astype(
                jnp.float32
            )
            if is_final:
                total = total * (1.0 / replicas)
            result[index, here] = total.astype(jnp.bfloat16)

    def finish(chunk, stage):
        stage_copy(chunk, stage).wait()
        if stage < bit_count:
            add(chunk, stage)
        if stage + 1 < stage_count:
            stage_copy(chunk, stage + 1).start()
        else:
            store_copy(chunk).start()

    def weight_term(chunk):
        which = 1 - chunk // chunks_per_array
        index = chunk // chunks_per_array

        @pl.loop(0, chunk_rows // TERM_BLOCK)
        def _(step):
            here = pl.ds(
                pl.multiple_of(base(chunk) + step * TERM_BLOCK, TERM_BLOCK), TERM_BLOCK
            )
            term = contract(normed[:, here], grads[which], 0, 0)
            held[index, here] = term.astype(jnp.bfloat16)

    is_last = jnp.where(section == sections - 1, 1.0, 0.0)

    def input_term():
        row_dot[...] = jnp.zeros_like(row_dot)

        @pl.loop(0, feature_blocks)
        def _(block):
            here = pl.ds(pl.multiple_of(block * FEATURE_BLOCK, FEATURE_BLOCK), FEATURE_BLOCK)
            grad_norm = contract(grads[0], weights[0, here], 1, 1)
            grad_norm = grad_norm + contract(grads[1], weights[1, here], 1, 1)
            part = gain[:, here] * grad_norm
            scaled[:, here] = part
            row_dot[...] += jnp.sum(
                x_held[:, here].astype(jnp.float32) * part, axis=-1, keepdims=True
            )

        top_copy.wait()

        @pl.loop(0, tokens // ROW_TILE)
        def _(step):
            here = pl.ds(pl.multiple_of(step * ROW_TILE, ROW_TILE), ROW_TILE)
            inverse = inv_rms[here]
            pull = inverse * inverse * inverse * (row_dot[here] * (1.0 / width))
            total = inverse * scaled[here] - x_held[here].astype(jnp.float32) * pull
            total = total + top[here].astype(jnp.float32) * is_last
            scaled[here] = total
            outgoing[here] = total.astype(jnp.bfloat16)

        cot_copy.start()

    final_copy = pltpu.make_async_copy(final, input_out.at[0], load_sem.at[3])

    def final_sum():
        cot_copy.wait()

        @pl.loop(0, tokens // ROW_TILE)
        def _(step):
            here = pl.ds(pl.multiple_of(step * ROW_TILE, ROW_TILE), ROW_TILE)
            total = scaled[here] + received[here].astype(jnp.float32) * (1.0 - is_last)
            final[here] = total.astype(jnp.bfloat16)

        final_copy.start()

    lags = [2 + 2 * stage if stage else 1 for stage in range(stage_count)]
    for step in range(chunk_count + lags[-1]):
        for stage in reversed(range(stage_count)):
            chunk = step - lags[stage]
            if 0 <= chunk < chunk_count:
                finish(chunk, stage)
        if step < chunk_count:
            weight_term(step)
            stage_copy(step, 0).start()
        if step == KEY_PASS_STEP:
            project(1)
            key_pass()
        if step == INPUT_TERM_STEP:
            input_term()
        if step == FINAL_SUM_STEP:
            final_sum()
    final_copy.wait()
    for chunk in range(chunk_count):
        store_copy(chunk).wait()


def per_device(layer_inputs, norm_gain, queries, output_gradient, w_key, value_matrix, top_grad):
    replicas = lax.axis_size("dp")
    sections = lax.axis_size("section")
    tokens, width = layer_inputs.shape[1:]
    rows, columns = w_key.shape[1:]
    bit_count = replicas.bit_length() - 1
    chunk_count = 2 * chunks_of(rows, replicas)
    low = jnp.bfloat16
    wide = jnp.float32
    anywhere = pl.BlockSpec(memory_space=pl.ANY)
    whole = pl.BlockSpec(memory_space=pltpu.VMEM)
    return pl.pallas_call(
        lambda *refs: whole_kernel(replicas, sections, *refs),
        out_shape=(
            jax.ShapeDtypeStruct(w_key.shape, low),
            jax.ShapeDtypeStruct(value_matrix.shape, low),
            jax.ShapeDtypeStruct(layer_inputs.shape, low),
        ),
        in_specs=[anywhere, whole] + [anywhere] * 5,
        out_specs=(anywhere,) * 3,
        scratch_shapes=[
            pltpu.VMEM((tokens, width), low),
            pltpu.VMEM((tokens, width), low),
            pltpu.VMEM((tokens, 1), wide),
            pltpu.VMEM(queries.shape[1:], low),
            pltpu.VMEM(queries.shape[1:], low),
            pltpu.VMEM((2, rows, columns), low),
            pltpu.VMEM((tokens, width), low),
            pltpu.VMEM((tokens, columns), wide),
            pltpu.VMEM((2, tokens, columns), low),
            pltpu.VMEM((2, tokens, columns), low),
            pltpu.VMEM((tokens, width), wide),
            pltpu.VMEM((tokens, 1), wide),
            pltpu.VMEM(
                (
                    tokens // SEQUENCE_TOKENS * KEY_VALUE_HEADS,
                    queries.shape[2] // columns * SEQUENCE_TOKENS,
                    SEQUENCE_TOKENS,
                ),
                wide,
            ),
            pltpu.VMEM((tokens, width), low),
            pltpu.VMEM((tokens, width), low),
            pltpu.VMEM((tokens, width), low),
            pltpu.VMEM((2, rows, columns), low),
            pltpu.VMEM((2, rows, columns), low),
        ]
        + [pltpu.VMEM((2 * rows >> (stage + 1), columns), low) for stage in range(bit_count)]
        + [
            pltpu.SemaphoreType.DMA((chunk_count, 2 * bit_count)),
            pltpu.SemaphoreType.DMA((chunk_count, 2 * bit_count)),
            pltpu.SemaphoreType.DMA((chunk_count,)),
            pltpu.SemaphoreType.DMA((2,)),
            pltpu.SemaphoreType.DMA((LOAD_PIECES,)),
            pltpu.SemaphoreType.DMA((2, width // FEATURE_BLOCK)),
            pltpu.SemaphoreType.DMA((4,)),
        ],
        compiler_params=pltpu.CompilerParams(
            collective_id=0, has_side_effects=True, vmem_limit_bytes=60 * 1024 * 1024
        ),
    )(layer_inputs, norm_gain, queries, output_gradient, w_key, value_matrix, top_grad)


def solution(mesh):
    in_specs = (
        P("section", "dp", None),
        P("section", None),
        P("section", "dp", None),
        P("section", "dp", None),
        P("section", None, None),
        P("section", None, None),
        P("dp", None),
    )
    out_specs = (P("section", None, None), P("section", None, None), P("section", "dp", None))
    return jax.shard_map(
        per_device, mesh=mesh, in_specs=in_specs, out_specs=out_specs, check_vma=False
    )
```
